32 devices in a mesh: space: 8 (over z, x), rad: 4 (over y, core).
Axes of the slice: x: 2, y: 2, z: 4, core: 2. Of those that a mesh axis runs over, the one named last changes fastest.
Arguments:
- cell_bin: int32 [524288], P(('space', 'rad')), may hold values from 0 to 255
- cell_fields: float32 [3, 524288], P(None, ('space', 'rad')), may hold values from 0.0005 to 0.005
- tile_halo: int32 [4096], P(('space', 'rad')), may hold values from 0 to 255, as said below
- halo_owner: int32 [256], replicated, may hold values from 0 to 7, as said below
Outputs:
- enclosed_mass: float32 [256, 256], P('space', 'rad')
- enclosed_volume: float32 [256, 256], P('space', 'rad')
- cumulative_entropy: float32 [256, 256], P('space', 'rad')
- circular_velocity: float32 [256, 256], P('space', 'rad')
The draws below stay inside these ranges and needn't reach their ends.
Inputs may be any that keep to these rules, and one draw needn't show every extreme that they name: `tile_halo`: the tiles of one device are in nondecreasing halo order; they go to exactly 4 owners, 32 tiles to each; the tiles of one device with one owner hold at most 16 distinct halos, and on every device some owner receives exactly 16. `halo_owner`: each index of space owns 32 consecutive halo ids.
All inputs are finite; a program needn't handle non-finite values.
Results may differ from the reference program's by a relative error of at most 0.000067.
Values sent between devices are 32-bit elements; how exact they have to be, the bound alone decides.
No kernel may reach another device: no remote copies, remote signals or barrier semaphores. Data moves between devices by JAX's collectives and lax.ppermute only.
A program may use at most 64 MiB of HBM per device.

```python
import math
import jax
import jax.numpy as jnp

TILE = 128
BINS = 256
HALO_DEV = 32
HALOS = 256
CAP = 32
HCAP = 16
DESTS = 4
CELLS = 524288
N_SPACE = 8
N_RAD = 4


def layout(key):
    block_perm = jax.random.permutation(jax.random.fold_in(key, 11), N_SPACE).astype(jnp.int32)
    owner = jnp.repeat(block_perm, HALO_DEV)
    inverse = jnp.argsort(block_perm).astype(jnp.int32)

    def one_device(dkey):
        first, second, third, fourth = jax.random.split(dkey, 4)
        targets = jax.random.permutation(first, N_SPACE)[:DESTS].astype(jnp.int32)
        counts = jax.random.randint(second, (DESTS,), 1, HCAP + 1).at[0].set(HCAP)
        chosen = jax.vmap(lambda k: jax.random.permutation(k, HALO_DEV)[:HCAP])(jax.random.split(third, DESTS))
        extra = jax.random.randint(fourth, (DESTS, CAP), 0, HCAP) % counts[:, None]
        column = jnp.arange(CAP, dtype=jnp.int32)[None, :]
        slot_index = jnp.where(column < counts[:, None], column, extra)
        halo_local = jnp.take_along_axis(chosen, slot_index, axis=1)
        halos = inverse[targets][:, None] * HALO_DEV + halo_local
        return jnp.sort(halos.reshape(-1)).astype(jnp.int32)
    device_keys = jax.random.split(jax.random.fold_in(key, 12), N_SPACE * N_RAD)
    tiles = jax.vmap(one_device)(device_keys).reshape(-1)
    return (owner, tiles)


def draw_tile_halo(key, part):
    return layout(key)[1]


def draw_halo_owner(key, part):
    return layout(key)[0]


def plant(array, stream_key, smallest, largest):
    shape = array.shape
    spot = [jax.random.randint(jax.random.fold_in(stream_key, axis), (), 0, shape[axis]) for axis in range(len(shape))]
    array = array.at[tuple(spot)].set(smallest)
    longest = shape.index(max(shape))
    spot[longest] = (spot[longest] + 1) % shape[longest]
    return array.at[tuple(spot)].set(largest)


def block_levels(key, extent, shards, low, high):
    loudness = 1.0
    for dim, blocks in shards:
        steps = jax.random.uniform(jax.random.fold_in(jax.random.fold_in(key, 6), dim), (blocks,), jnp.float32, low / len(shards), high / len(shards))
        loudness = loudness * jnp.repeat(jnp.exp(steps), extent[dim] // blocks).reshape((-1,) + (1,) * (len(extent) - 1 - dim))
    return loudness


def setup_inputs(seed: int = 0) -> dict:
    key_list = jax.random.split(jax.random.key(seed), 5)
    return {
        "cell_bin": plant(jax.random.randint(key_list[0], (CELLS,), 0, BINS), jax.random.fold_in(key_list[0], 1), 0, BINS - 1).astype(jnp.int32),
        "cell_fields": jnp.clip(jnp.exp(math.log(0.005) - 2.30258502 * jax.random.uniform(key_list[1], (3, CELLS), jnp.float32) ** block_levels(key_list[1], (3, CELLS), ((1, 32),), -0.2, 0.2)), 0.0005, 0.005),
        "tile_halo": draw_tile_halo(jax.random.fold_in(key_list[4], 71), 0),
        "halo_owner": draw_halo_owner(jax.random.fold_in(key_list[4], 71), 0),
    }


log_inner = -2.302585092994046

def reference(cell_bin, cell_fields, tile_halo, halo_owner):
    cell_halo = jnp.repeat(tile_halo, TILE)
    segment = cell_halo * BINS + cell_bin
    binned = jax.ops.segment_sum(cell_fields.T, segment, num_segments=HALOS * BINS)
    binned = binned.reshape(HALOS, BINS, 3)
    running = jnp.cumsum(binned, axis=1)
    ranking = jnp.argsort(halo_owner, stable=True)
    running = running[ranking]
    position = (jnp.arange(BINS) + 1).astype(jnp.float32)
    radius = jnp.exp(log_inner + position * (-log_inner / BINS))
    enclosed = running[:, :, 0]
    velocity = jnp.sqrt(enclosed / radius[None, :])
    return (enclosed, running[:, :, 1], running[:, :, 2], velocity)
```

```python
import functools
import math

import jax
import jax.numpy as jnp
from jax import lax
from jax.experimental import pallas as pl
from jax.experimental.pallas import tpu as pltpu
from jax.sharding import PartitionSpec as P

TILE = 128
BINS = 256
LANES = 128
PACK = 16
CHUNK = 8
BATCH = 32
VMEM_LIMIT = 16 * 1024 * 1024

log_inner = -2.302585092994046


def split(x):
    hi = x.astype(jnp.bfloat16).astype(jnp.float32)
    return hi, x - hi


def bin_kernel(spaces, rads, per, slots, rows, owner_ref, halo_ref, bin_ref, field_ref, out_ref):
    tiles = bin_ref.shape[0]
    halo_dev = owner_ref.shape[0] // spaces
    bin_dev = BINS // rads
    parts = LANES // bin_dev
    sub = slots // parts
    one, zero = jnp.bfloat16(1), jnp.bfloat16(0)
    bin_ids = [
        (lax.broadcasted_iota(jnp.int32, (PACK, LANES), 0) + k * PACK).astype(jnp.float32).astype(jnp.bfloat16)
        for k in range(BINS // PACK)
    ]
    slot_ids = lax.broadcasted_iota(jnp.int32, (slots, LANES), 0)
    lane = lax.broadcasted_iota(jnp.int32, (1, LANES), 1)

    @pl.loop(0, spaces * rads)
    def _(block):
        out_ref[pl.ds(block * rows, rows - 1), 0, :] = jnp.zeros((rows - 1, LANES), jnp.float32)
        out_ref[block * rows + rows - 1] = jnp.full((1, LANES), -1.0, jnp.float32)

    @pl.loop(0, tiles // per)
    def _(group):
        owner = owner_ref[halo_ref[group * per]]
        slot = jnp.int32(0)
        places = jnp.full((1, LANES), -1, jnp.int32)
        total = None
        for chunk in range(0, per, CHUNK):
            steps, values = [], []
            for k in range(chunk, min(chunk + CHUNK, per)):
                t = group * per + k
                halo = halo_ref[t]
                if k:
                    slot = slot + (halo != halo_ref[t - 1]).astype(jnp.int32)
                local = lax.rem(halo, halo_dev)
                places = jnp.where(lane == (slot // sub) * bin_dev + local, lax.rem(slot, sub), places)
                label = jnp.broadcast_to(bin_ref[pl.ds(t, 1), :], (PACK, LANES))
                label = label.astype(jnp.float32).astype(jnp.bfloat16)
                steps.append(jnp.concatenate([jnp.where(label <= ids, one, zero) for ids in bin_ids], axis=0))
                chosen = slot_ids == slot
                pieces = []
                for f in range(3):
                    cells = pl.ds(pl.multiple_of(t * TILE, TILE), TILE)
                    for piece in split(field_ref[f : f + 1, cells]):
                        spread = jnp.broadcast_to(piece, (slots, LANES))
                        pieces.append(jnp.where(chosen, spread, 0.0).astype(jnp.bfloat16))
                values.append(jnp.concatenate(pieces, axis=0))
            step = jnp.concatenate(steps, axis=1)
            value = jnp.concatenate(values, axis=1)
            part = lax.dot_general(
                value, step, (((1,), (1,)), ((), ())), preferred_element_type=jnp.float32
            )
            total = part if total is None else total + part
        for f in range(3):
            running = total[2 * f * slots : (2 * f + 1) * slots] + total[(2 * f + 1) * slots : (2 * f + 2) * slots]
            for r in range(rads):
                packed = jnp.concatenate(
                    [running[a * sub : (a + 1) * sub, r * bin_dev : (r + 1) * bin_dev] for a in range(parts)], axis=1
                )
                base = (owner * rads + r) * rows + f * sub
                out_ref[pl.ds(base, sub), 0, :] = packed
        for r in range(rads):
            out_ref[(owner * rads + r) * rows + rows - 1] = places.astype(jnp.float32)


def merge_kernel(halo_dev, bin_dev, sub, rows, got_ref, mass_ref, volume_ref, entropy_ref, speed_ref):
    sources = got_ref.shape[0] // rows
    batch = math.gcd(sources, BATCH)
    row_ids = lax.broadcasted_iota(jnp.int32, (sub, LANES), 0).astype(jnp.float32)

    def add(first):
        picks, values = [], []
        for i in range(batch):
            base = (first + i) * rows
            places = jnp.broadcast_to(got_ref[base + rows - 1], (sub, LANES))
            picks.append((places == row_ids).astype(jnp.float32))
            pieces = []
            for f in range(3):
                pieces.extend(split(got_ref[pl.ds(base + f * sub, sub), 0, :]))
            values.append(jnp.concatenate(pieces, axis=1))
        pick = jnp.concatenate(picks, axis=0).astype(jnp.bfloat16)
        value = jnp.concatenate(values, axis=0).astype(jnp.bfloat16)
        return lax.dot_general(pick, value, (((0,), (0,)), ((), ())), preferred_element_type=jnp.float32)

    sums = lax.fori_loop(1, sources // batch, lambda k, acc: acc + add(k * batch), add(0))
    results = []
    for f in range(3):
        both = sums[:, 2 * f * LANES : (2 * f + 1) * LANES] + sums[:, (2 * f + 1) * LANES : (2 * f + 2) * LANES]
        acc = None
        for a in range(LANES // bin_dev):
            part = both[a * bin_dev : a * bin_dev + halo_dev, a * bin_dev : (a + 1) * bin_dev]
            acc = part if acc is None else acc + part
        results.append(acc)
    mass_ref[...], volume_ref[...], entropy_ref[...] = results
    first = lax.axis_index("rad") * bin_dev + 1
    position = (lax.broadcasted_iota(jnp.int32, (1, bin_dev), 1) + first).astype(jnp.float32)
    radius = jnp.exp(log_inner + position * (-log_inner / BINS))
    speed_ref[...] = jnp.sqrt(results[0] / radius)


def body(cell_bin, cell_fields, tile_halo, halo_owner):
    spaces = lax.axis_size("space")
    rads = lax.axis_size("rad")
    bin_dev = BINS // rads
    tiles = tile_halo.shape[0]
    halo_dev = halo_owner.shape[0] // spaces
    per = max(2, 2 * tiles // spaces)
    slots = -(-max(1, per // 2) // PACK) * PACK
    sub = slots * bin_dev // LANES
    rows = 3 * sub + 1
    vmem = pl.BlockSpec(memory_space=pltpu.VMEM)
    smem = pl.BlockSpec(memory_space=pltpu.SMEM)
    outgoing = pl.pallas_call(
        functools.partial(bin_kernel, spaces, rads, per, slots, rows),
        out_shape=jax.ShapeDtypeStruct((spaces * rads * rows, 1, LANES), jnp.float32),
        in_specs=[smem, smem, vmem, vmem],
        out_specs=vmem,
        compiler_params=pltpu.CompilerParams(vmem_limit_bytes=VMEM_LIMIT),
    )(halo_owner, tile_halo, cell_bin.reshape(tiles, TILE), cell_fields)
    received = lax.all_to_all(
        outgoing.reshape(spaces * rads, rows, 1, LANES), ("space", "rad"), split_axis=0, concat_axis=0, tiled=True
    )
    return pl.pallas_call(
        functools.partial(merge_kernel, halo_dev, bin_dev, sub, rows),
        out_shape=[jax.ShapeDtypeStruct((halo_dev, bin_dev), jnp.float32)] * 4,
        in_specs=[vmem],
        out_specs=[vmem] * 4,
        compiler_params=pltpu.CompilerParams(vmem_limit_bytes=VMEM_LIMIT),
    )(received.reshape(spaces * rads * rows, 1, LANES))


def solution(mesh):
    in_specs = (P(("space", "rad")), P(None, ("space", "rad")), P(("space", "rad")), P())
    out_specs = (P("space", "rad"), P("space", "rad"), P("space", "rad"), P("space", "rad"))
    return jax.shard_map(body, mesh=mesh, in_specs=in_specs, out_specs=out_specs, check_vma=False)
```

```python
import functools
import math

import jax
import jax.numpy as jnp
from jax import lax
from jax.experimental import pallas as pl
from jax.experimental.pallas import tpu as pltpu
from jax.sharding import PartitionSpec as P

TILE = 128
BINS = 256
LANES = 128
PACK = 16
FIELDS = 4
BATCH = 32
VMEM_LIMIT = 16 * 1024 * 1024

log_inner = -2.302585092994046


def divide(x, n):
    if n & (n - 1):
        return lax.div(x, jnp.full_like(x, n)), lax.rem(x, jnp.full_like(x, n))
    return lax.shift_right_logical(x, jnp.full_like(x, n.bit_length() - 1)), x & (n - 1)


def iota(shape, dim):
    return lax.broadcasted_iota(jnp.int32, shape, dim)


def root_of(devices):
    return devices // 4 + 1


def matmul(a, b, contract):
    return lax.dot_general(a, b, ((contract, contract), ((), ())), preferred_element_type=jnp.float32)


def bin_kernel(
    spaces, rads, per, slots, rows,
    owner_hbm, halo_hbm, line_hbm, bin_hbm, field_hbm, out_ref,
    owner_ref, halo_ref, line_ref, bin_ref, field_ref, place_ref, acc_ref, sem,
):
    tiles = bin_ref.shape[0]
    halo_dev = owner_ref.shape[0] // spaces
    bin_dev = BINS // rads
    parts = LANES // bin_dev
    sub = slots // parts
    lead = FIELDS * rads
    root = root_of(spaces * rads)
    copies = [
        pltpu.make_async_copy(source, target, sem.at[k])
        for k, (source, target) in enumerate(
            [(line_hbm, line_ref), (halo_hbm, halo_ref), (owner_hbm, owner_ref), (bin_hbm, bin_ref), (field_hbm, field_ref)]
        )
    ]
    for copy in copies:
        copy.start()

    @pl.loop(0, spaces * rads)
    def _(block):
        out_ref[pl.ds(block * rows, rows - 1), :] = jnp.zeros((rows - 1, LANES), jnp.float32)
        out_ref[pl.ds(block * rows + rows - 1, 1), :] = jnp.full((1, LANES), -1.0, jnp.float32)

    for copy in copies[:1]:
        copy.wait()
    line = jnp.broadcast_to(line_ref[...], (8, tiles))
    start = (line != pltpu.roll(line, 1, 1)) | (divide(iota((8, tiles), 1), per)[1] == 0)
    start = jnp.broadcast_to(jnp.where(start, 1.0, 0.0)[:1], (tiles, tiles))
    local = jnp.broadcast_to(divide(line, halo_dev)[1].astype(jnp.float32)[:1], (tiles, tiles))
    down, across = iota((tiles, tiles), 0), iota((tiles, tiles), 1)
    before = (across <= down) & (divide(across, per)[0] == divide(down, per)[0])
    flat = jnp.concatenate([jnp.where(before, start, 0.0), jnp.where(across == down, local, 0.0)], axis=0)
    spread = lax.dot_general(
        flat.astype(jnp.bfloat16), jnp.ones((tiles, LANES), jnp.bfloat16), (((1,), (0,)), ((), ())),
        preferred_element_type=jnp.float32,
    )
    part, row = divide(spread[:tiles].astype(jnp.int32) - 1, sub)
    key = part * bin_dev + spread[tiles:].astype(jnp.int32)
    place_ref[...] = jnp.where(key == iota((tiles, LANES), 1), row, -1).astype(jnp.float32)

    one, zero = jnp.bfloat16(1), jnp.bfloat16(0)
    bin_ids = [
        (iota((PACK, LANES), 0) + k * PACK).astype(jnp.float32).astype(jnp.bfloat16) for k in range(bin_dev // PACK)
    ]
    field_id, range_id = divide(iota((lead, LANES), 0), rads)
    range_id = jnp.where(field_id < 3, range_id, -1)
    empty = jnp.zeros((2 * lead, LANES), jnp.bfloat16)

    for copy in copies[1:]:
        copy.wait()

    @pl.loop(0, tiles // per)
    def _(group):
        acc_ref[...] = jnp.zeros_like(acc_ref)
        owner = owner_ref[halo_ref[group * per]]
        slot = jnp.int32(0)
        carry = None
        width = math.gcd(per, 2)
        for first in range(0, per, width):
            values, steps = [], []
            for k in range(first, first + width):
                t = group * per + k
                span, low = divide(bin_ref[pl.ds(t, 1), :], bin_dev)
                cells = pl.ds(pl.multiple_of(t * TILE, TILE), TILE)
                field = [jnp.broadcast_to(field_ref[f : f + 1, cells], (lead, LANES)) for f in range(3)]
                value = jnp.where(field_id == 0, field[0], jnp.where(field_id == 1, field[1], field[2]))
                value = jnp.where(jnp.broadcast_to(span, (lead, LANES)) == range_id, value, 0.0)
                high = value.astype(jnp.bfloat16)
                value = jnp.concatenate([high, (value - high.astype(jnp.float32)).astype(jnp.bfloat16)], axis=0)
                values.append(jnp.concatenate([empty] * (k - first) + [value] + [empty] * (first + width - 1 - k), axis=1))
                low = jnp.broadcast_to(low, (PACK, LANES)).astype(jnp.float32).astype(jnp.bfloat16)
                steps.append(jnp.concatenate([jnp.where(low <= ids, one, zero) for ids in bin_ids], axis=0))
            sums = matmul(jnp.concatenate(values, axis=0), jnp.concatenate(steps, axis=1), (1,))
            for k in range(first, first + width):
                at = (k - first) * 2 * lead
                tile_sum = sums[at : at + lead] + sums[at + lead : at + 2 * lead]
                if k:
                    fresh = halo_ref[group * per + k] != halo_ref[group * per + k - 1]
                    slot = slot + fresh.astype(jnp.int32)
                    carry = jnp.where(fresh, 0.0, carry) + tile_sum
                else:
                    carry = tile_sum
                acc_ref[pl.ds(pl.multiple_of(slot * lead, lead), lead), :bin_dev] = carry
        base = []
        for r in range(rads):
            block = owner * rads + r
            block = jnp.where(block == 0, root, jnp.where(block == root, 0, block))
            base.append(block * rows)
            places = jnp.max(place_ref[pl.ds(group * per, per), :], axis=0, keepdims=True)
            out_ref[pl.ds(base[r] + rows - 1, 1), :] = places
        for f in range(3):
            inner = [jnp.zeros((sub, bin_dev), jnp.float32)] * parts
            for r in range(rads):
                pieces = []
                for a in range(parts):
                    own = acc_ref[pl.ds(a * sub * lead + f * rads + r, sub, stride=lead), :][:, :bin_dev]
                    pieces.append(own + inner[a])
                    inner[a] = inner[a] + jnp.broadcast_to(own[:, bin_dev - 1 :], (sub, bin_dev))
                out_ref[pl.ds(base[r] + f * sub, sub), :] = jnp.concatenate(pieces, axis=1)


def merge_kernel(halo_dev, bin_dev, sub, rows, got_ref, mass_ref, volume_ref, entropy_ref, speed_ref):
    sources = got_ref.shape[0] // rows
    batch = math.gcd(sources, BATCH)
    row_ids = iota((sub, LANES), 0).astype(jnp.float32)

    def add(first):
        picks, values = [], []
        for i in range(batch):
            base = (first + i) * rows
            places = jnp.broadcast_to(got_ref[pl.ds(base + rows - 1, 1), :], (sub, LANES))
            picks.append((places == row_ids).astype(jnp.float32))
            pieces = []
            for f in range(3):
                value = got_ref[pl.ds(base + f * sub, sub), :]
                high = value.astype(jnp.bfloat16).astype(jnp.float32)
                pieces.extend([high, value - high])
            values.append(jnp.concatenate(pieces, axis=1))
        pick = jnp.concatenate(picks, axis=0).astype(jnp.bfloat16)
        value = jnp.concatenate(values, axis=0).astype(jnp.bfloat16)
        return matmul(pick, value, (0,))

    sums = lax.fori_loop(1, sources // batch, lambda k, acc: acc + add(k * batch), add(0))
    results = []
    for f in range(3):
        both = sums[:, 2 * f * LANES : (2 * f + 1) * LANES] + sums[:, (2 * f + 1) * LANES : (2 * f + 2) * LANES]
        acc = None
        for a in range(LANES // bin_dev):
            part = both[a * bin_dev : a * bin_dev + halo_dev, a * bin_dev : (a + 1) * bin_dev]
            acc = part if acc is None else acc + part
        results.append(acc)
    mass_ref[...], volume_ref[...], entropy_ref[...] = results
    first = lax.axis_index("rad") * bin_dev + 1
    position = (iota((1, bin_dev), 1) + first).astype(jnp.float32)
    radius = jnp.exp(log_inner + position * (-log_inner / BINS))
    speed_ref[...] = jnp.sqrt(results[0] / radius)


def body(cell_bin, cell_fields, tile_halo, halo_owner):
    spaces = lax.axis_size("space")
    rads = lax.axis_size("rad")
    bin_dev = BINS // rads
    tiles = tile_halo.shape[0]
    halo_dev = halo_owner.shape[0] // spaces
    per = max(2, 2 * tiles // spaces)
    slots = -(-max(1, per // 2) // PACK) * PACK
    sub = slots * bin_dev // LANES
    rows = 3 * sub + 1
    devices = spaces * rads
    vmem = pl.BlockSpec(memory_space=pltpu.VMEM)
    hbm = pl.BlockSpec(memory_space=pltpu.HBM)
    params = pltpu.CompilerParams(vmem_limit_bytes=VMEM_LIMIT)
    outgoing = pl.pallas_call(
        functools.partial(bin_kernel, spaces, rads, per, slots, rows),
        out_shape=jax.ShapeDtypeStruct((devices * rows, LANES), jnp.float32),
        in_specs=[hbm] * 5,
        out_specs=vmem,
        scratch_shapes=[
            pltpu.SMEM(halo_owner.shape, jnp.int32),
            pltpu.SMEM((tiles,), jnp.int32),
            pltpu.VMEM((1, tiles), jnp.int32),
            pltpu.VMEM((tiles, TILE), jnp.int32),
            pltpu.VMEM(cell_fields.shape, jnp.float32),
            pltpu.VMEM((tiles, LANES), jnp.float32),
            pltpu.VMEM((slots * FIELDS * rads, LANES), jnp.float32),
            pltpu.SemaphoreType.DMA((5,)),
        ],
        compiler_params=params,
    )(
        *[
            pltpu.with_memory_space_constraint(x, pltpu.HBM)
            for x in (halo_owner, tile_halo, tile_halo.reshape(1, tiles), cell_bin.reshape(tiles, TILE), cell_fields)
        ]
    )
    order = list(range(devices))
    order[0], order[root_of(devices)] = order[root_of(devices)], order[0]
    received = lax.all_to_all(
        outgoing.reshape(devices, rows, 1, LANES),
        ("space", "rad"),
        split_axis=0,
        concat_axis=0,
        axis_index_groups=[order],
        tiled=True,
    )
    return pl.pallas_call(
        functools.partial(merge_kernel, halo_dev, bin_dev, sub, rows),
        out_shape=[jax.ShapeDtypeStruct((halo_dev, bin_dev), jnp.float32)] * 4,
        in_specs=[vmem],
        out_specs=[vmem] * 4,
        compiler_params=params,
    )(received.reshape(devices * rows, LANES))


def solution(mesh):
    in_specs = (P(("space", "rad")), P(None, ("space", "rad")), P(("space", "rad")), P())
    out_specs = (P("space", "rad"), P("space", "rad"), P("space", "rad"), P("space", "rad"))
    return jax.shard_map(body, mesh=mesh, in_specs=in_specs, out_specs=out_specs, check_vma=False)
```

```python
import functools
import math

import jax
import jax.numpy as jnp
from jax import lax
from jax.experimental import pallas as pl
from jax.experimental.pallas import tpu as pltpu
from jax.sharding import PartitionSpec as P

TILE = 128
BINS = 256
LANES = 128
PACK = 16
FIELDS = 4
BATCH = 32
VMEM_LIMIT = 16 * 1024 * 1024

log_inner = -2.302585092994046


def divide(x, n):
    if n & (n - 1):
        return lax.div(x, jnp.full_like(x, n)), lax.rem(x, jnp.full_like(x, n))
    return lax.shift_right_logical(x, jnp.full_like(x, n.bit_length() - 1)), x & (n - 1)


def iota(shape, dim):
    return lax.broadcasted_iota(jnp.int32, shape, dim)


def root_of(members):
    return members - 1


def matmul(a, b, contract):
    return lax.dot_general(a, b, ((contract, contract), ((), ())), preferred_element_type=jnp.float32)


def bin_kernel(
    spaces, rads, per, slots, rows,
    owner_hbm, halo_hbm, line_hbm, bin_hbm, field_hbm, out_ref,
    owner_ref, halo_ref, line_ref, bin_ref, field_ref, place_ref, acc_ref, sem,
):
    tiles = bin_ref.shape[0]
    halo_dev = owner_ref.shape[0] // spaces
    bin_dev = BINS // rads
    parts = LANES // bin_dev
    sub = slots // parts
    lead = FIELDS * rads
    root = root_of(spaces * rads // 2)
    copies = [
        pltpu.make_async_copy(source, target, sem.at[k])
        for k, (source, target) in enumerate(
            [(line_hbm, line_ref), (halo_hbm, halo_ref), (owner_hbm, owner_ref), (bin_hbm, bin_ref), (field_hbm, field_ref)]
        )
    ]
    for copy in copies:
        copy.start()

    @pl.loop(0, spaces * rads)
    def _(block):
        out_ref[pl.ds(block * rows, rows - 1), :] = jnp.zeros((rows - 1, LANES), jnp.float32)
        out_ref[pl.ds(block * rows + rows - 1, 1), :] = jnp.full((1, LANES), -1.0, jnp.float32)

    for copy in copies[:1]:
        copy.wait()
    line = jnp.broadcast_to(line_ref[...], (8, tiles))
    start = (line != pltpu.roll(line, 1, 1)) | (divide(iota((8, tiles), 1), per)[1] == 0)
    start = jnp.broadcast_to(jnp.where(start, 1.0, 0.0)[:1], (tiles, tiles))
    local = jnp.broadcast_to(divide(line, halo_dev)[1].astype(jnp.float32)[:1], (tiles, tiles))
    down, across = iota((tiles, tiles), 0), iota((tiles, tiles), 1)
    before = (across <= down) & (divide(across, per)[0] == divide(down, per)[0])
    flat = jnp.concatenate([jnp.where(before, start, 0.0), jnp.where(across == down, local, 0.0)], axis=0)
    spread = lax.dot_general(
        flat.astype(jnp.bfloat16), jnp.ones((tiles, LANES), jnp.bfloat16), (((1,), (0,)), ((), ())),
        preferred_element_type=jnp.float32,
    )
    part, row = divide(spread[:tiles].astype(jnp.int32) - 1, sub)
    key = part * bin_dev + spread[tiles:].astype(jnp.int32)
    place_ref[...] = jnp.where(key == iota((tiles, LANES), 1), row, -1).astype(jnp.float32)

    one, zero = jnp.bfloat16(1), jnp.bfloat16(0)
    bin_ids = [
        (iota((PACK, LANES), 0) + k * PACK).astype(jnp.float32).astype(jnp.bfloat16) for k in range(bin_dev // PACK)
    ]
    field_id, range_id = divide(iota((lead, LANES), 0), rads)
    range_id = jnp.where(field_id < 3, range_id, -1)
    empty = jnp.zeros((2 * lead, LANES), jnp.bfloat16)

    for copy in copies[1:]:
        copy.wait()

    @pl.loop(0, tiles // per)
    def _(group):
        acc_ref[...] = jnp.zeros_like(acc_ref)
        owner = owner_ref[halo_ref[group * per]]
        slot = jnp.int32(0)
        carry = None
        width = math.gcd(per, 2)
        for first in range(0, per, width):
            values, steps = [], []
            for k in range(first, first + width):
                t = group * per + k
                span, low = divide(bin_ref[pl.ds(t, 1), :], bin_dev)
                cells = pl.ds(pl.multiple_of(t * TILE, TILE), TILE)
                field = [jnp.broadcast_to(field_ref[f : f + 1, cells], (lead, LANES)) for f in range(3)]
                value = jnp.where(field_id == 0, field[0], jnp.where(field_id == 1, field[1], field[2]))
                value = jnp.where(jnp.broadcast_to(span, (lead, LANES)) == range_id, value, 0.0)
                high = value.astype(jnp.bfloat16)
                value = jnp.concatenate([high, (value - high.astype(jnp.float32)).astype(jnp.bfloat16)], axis=0)
                values.append(jnp.concatenate([empty] * (k - first) + [value] + [empty] * (first + width - 1 - k), axis=1))
                low = jnp.broadcast_to(low, (PACK, LANES)).astype(jnp.float32).astype(jnp.bfloat16)
                steps.append(jnp.concatenate([jnp.where(low <= ids, one, zero) for ids in bin_ids], axis=0))
            sums = matmul(jnp.concatenate(values, axis=0), jnp.concatenate(steps, axis=1), (1,))
            for k in range(first, first + width):
                at = (k - first) * 2 * lead
                tile_sum = sums[at : at + lead] + sums[at + lead : at + 2 * lead]
                if k:
                    fresh = halo_ref[group * per + k] != halo_ref[group * per + k - 1]
                    slot = slot + fresh.astype(jnp.int32)
                    carry = jnp.where(fresh, 0.0, carry) + tile_sum
                else:
                    carry = tile_sum
                acc_ref[pl.ds(pl.multiple_of(slot * lead, lead), lead), :bin_dev] = carry
        base = []
        side = lax.div(owner, spaces // 2)
        for r in range(rads):
            place = lax.rem(owner, spaces // 2) * rads + r
            place = jnp.where(place == root, 0, place + (place < root).astype(jnp.int32))
            base.append((2 * place + side) * rows)
            places = jnp.max(place_ref[pl.ds(group * per, per), :], axis=0, keepdims=True)
            out_ref[pl.ds(base[r] + rows - 1, 1), :] = places
        for f in range(3):
            inner = [jnp.zeros((sub, bin_dev), jnp.float32)] * parts
            for r in range(rads):
                pieces = []
                for a in range(parts):
                    own = acc_ref[pl.ds(a * sub * lead + f * rads + r, sub, stride=lead), :][:, :bin_dev]
                    pieces.append(own + inner[a])
                    inner[a] = inner[a] + jnp.broadcast_to(own[:, bin_dev - 1 :], (sub, bin_dev))
                out_ref[pl.ds(base[r] + f * sub, sub), :] = jnp.concatenate(pieces, axis=1)


def fold(x, height):
    return jnp.concatenate([x[k : k + height] for k in range(0, x.shape[0], height)], axis=1)


def merge_kernel(halo_dev, bin_dev, sub, rows, got_ref, own_ref, other_ref):
    sources = got_ref.shape[0] // (2 * rows)
    batch = math.gcd(sources, BATCH)
    row_ids = iota((sub, LANES), 0).astype(jnp.float32)

    def add(side, first):
        picks, values = [], []
        for i in range(batch):
            base = (2 * (first + i) + side) * rows
            places = jnp.broadcast_to(got_ref[pl.ds(base + rows - 1, 1), :], (sub, LANES))
            picks.append((places == row_ids).astype(jnp.float32))
            pieces = []
            for f in range(3):
                value = got_ref[pl.ds(base + f * sub, sub), :]
                high = value.astype(jnp.bfloat16).astype(jnp.float32)
                pieces.extend([high, value - high])
            values.append(jnp.concatenate(pieces, axis=1))
        pick = jnp.concatenate(picks, axis=0).astype(jnp.bfloat16)
        value = jnp.concatenate(values, axis=0).astype(jnp.bfloat16)
        return matmul(pick, value, (0,))

    results = []
    for side in range(2):
        sums = lax.fori_loop(
            1, sources // batch, lambda k, acc, side=side: acc + add(side, k * batch), add(side, 0)
        )
        fields = []
        for f in range(3):
            both = sums[:, 2 * f * LANES : (2 * f + 1) * LANES] + sums[:, (2 * f + 1) * LANES : (2 * f + 2) * LANES]
            acc = None
            for a in range(LANES // bin_dev):
                part = both[a * bin_dev : a * bin_dev + halo_dev, a * bin_dev : (a + 1) * bin_dev]
                acc = part if acc is None else acc + part
            fields.append(fold(acc, halo_dev // (LANES // bin_dev)))
        results.append(jnp.concatenate(fields, axis=0))
    first = lax.axis_index("space") < lax.axis_size("space") // 2
    own_ref[...] = jnp.where(first, results[0], results[1])
    other_ref[...] = jnp.where(first, results[1], results[0])


def finish_kernel(halo_dev, bin_dev, own_ref, got_ref, mass_ref, volume_ref, entropy_ref, speed_ref):
    total = own_ref[...] + got_ref[...]
    height = halo_dev * bin_dev // LANES
    total = [
        jnp.concatenate(
            [total[f * height : (f + 1) * height, a : a + bin_dev] for a in range(0, LANES, bin_dev)], axis=0
        )
        for f in range(3)
    ]
    mass_ref[...], volume_ref[...], entropy_ref[...] = total
    first = lax.axis_index("rad") * bin_dev + 1
    position = (iota((1, bin_dev), 1) + first).astype(jnp.float32)
    radius = jnp.exp(log_inner + position * (-log_inner / BINS))
    speed_ref[...] = jnp.sqrt(total[0] / radius)


def body(cell_bin, cell_fields, tile_halo, halo_owner):
    spaces = lax.axis_size("space")
    rads = lax.axis_size("rad")
    bin_dev = BINS // rads
    tiles = tile_halo.shape[0]
    halo_dev = halo_owner.shape[0] // spaces
    per = max(2, 2 * tiles // spaces)
    slots = -(-max(1, per // 2) // PACK) * PACK
    sub = slots * bin_dev // LANES
    rows = 3 * sub + 1
    devices = spaces * rads
    vmem = pl.BlockSpec(memory_space=pltpu.VMEM)
    hbm = pl.BlockSpec(memory_space=pltpu.HBM)
    params = pltpu.CompilerParams(vmem_limit_bytes=VMEM_LIMIT)
    outgoing = pl.pallas_call(
        functools.partial(bin_kernel, spaces, rads, per, slots, rows),
        out_shape=jax.ShapeDtypeStruct((devices * rows, LANES), jnp.float32),
        in_specs=[hbm] * 5,
        out_specs=vmem,
        scratch_shapes=[
            pltpu.SMEM(halo_owner.shape, jnp.int32),
            pltpu.SMEM((tiles,), jnp.int32),
            pltpu.VMEM((1, tiles), jnp.int32),
            pltpu.VMEM((tiles, TILE), jnp.int32),
            pltpu.VMEM(cell_fields.shape, jnp.float32),
            pltpu.VMEM((tiles, LANES), jnp.float32),
            pltpu.VMEM((slots * FIELDS * rads, LANES), jnp.float32),
            pltpu.SemaphoreType.DMA((5,)),
        ],
        compiler_params=params,
    )(
        *[
            pltpu.with_memory_space_constraint(x, pltpu.HBM)
            for x in (halo_owner, tile_halo, tile_halo.reshape(1, tiles), cell_bin.reshape(tiles, TILE), cell_fields)
        ]
    )
    root = root_of(devices // 2)
    order = [root] + [k for k in range(devices // 2) if k != root]
    received = lax.all_to_all(
        outgoing.reshape(devices // 2, 2 * rows, 1, LANES),
        ("space", "rad"),
        split_axis=0,
        concat_axis=0,
        axis_index_groups=[[side * (devices // 2) + k for k in order] for side in range(2)],
        tiled=True,
    )
    own, other = pl.pallas_call(
        functools.partial(merge_kernel, halo_dev, bin_dev, sub, rows),
        out_shape=[jax.ShapeDtypeStruct((3 * halo_dev * bin_dev // LANES, LANES), jnp.float32)] * 2,
        in_specs=[vmem],
        out_specs=[vmem] * 2,
        compiler_params=params,
    )(received.reshape(devices * rows, LANES))
    got = lax.ppermute(other, "space", [(s, (s + spaces // 2) % spaces) for s in range(spaces)])
    return pl.pallas_call(
        functools.partial(finish_kernel, halo_dev, bin_dev),
        out_shape=[jax.ShapeDtypeStruct((halo_dev, bin_dev), jnp.float32)] * 4,
        in_specs=[vmem] * 2,
        out_specs=[vmem] * 4,
        compiler_params=params,
    )(own, got)


def solution(mesh):
    in_specs = (P(("space", "rad")), P(None, ("space", "rad")), P(("space", "rad")), P())
    out_specs = (P("space", "rad"), P("space", "rad"), P("space", "rad"), P("space", "rad"))
    return jax.shard_map(body, mesh=mesh, in_specs=in_specs, out_specs=out_specs, check_vma=False)
```

```python
import functools
import math

import jax
import jax.numpy as jnp
from jax import lax
from jax.experimental import pallas as pl
from jax.experimental.pallas import tpu as pltpu
from jax.sharding import PartitionSpec as P

TILE = 128
BINS = 256
LANES = 128
PACK = 16
FIELDS = 4
UNROLL = 4
BATCH = 32
VMEM_LIMIT = 16 * 1024 * 1024

log_inner = -2.302585092994046


def divide(x, n):
    if n & (n - 1):
        return lax.div(x, jnp.full_like(x, n)), lax.rem(x, jnp.full_like(x, n))
    return lax.shift_right_logical(x, jnp.full_like(x, n.bit_length() - 1)), x & (n - 1)


def iota(shape, dim):
    return lax.broadcasted_iota(jnp.int32, shape, dim)


def matmul(a, b, contract):
    return lax.dot_general(a, b, ((contract, contract), ((), ())), preferred_element_type=jnp.float32)


def bin_kernel(
    spaces, rads, per, slots, rows,
    owner_hbm, halo_hbm, line_hbm, bin_hbm, field_hbm, out_ref,
    owner_ref, halo_ref, line_ref, bin_ref, field_ref, place_ref, acc_ref, sem,
):
    tiles = bin_ref.shape[0]
    halo_dev = owner_ref.shape[0] // spaces
    bin_dev = BINS // rads
    parts = LANES // bin_dev
    sub = slots // parts
    lead = FIELDS * rads
    copies = [
        pltpu.make_async_copy(source, target, sem.at[k])
        for k, (source, target) in enumerate(
            [(line_hbm, line_ref), (halo_hbm, halo_ref), (owner_hbm, owner_ref), (bin_hbm, bin_ref), (field_hbm, field_ref)]
        )
    ]
    for copy in copies:
        copy.start()

    @pl.loop(0, spaces * rads)
    def _(block):
        out_ref[pl.ds(block * rows, rows - 1), :] = jnp.zeros((rows - 1, LANES), jnp.float32)
        out_ref[pl.ds(block * rows + rows - 1, 1), :] = jnp.full((1, LANES), -1.0, jnp.float32)

    for copy in copies[:1]:
        copy.wait()
    line = jnp.broadcast_to(line_ref[...], (8, tiles))
    start = (line != pltpu.roll(line, 1, 1)) | (divide(iota((8, tiles), 1), per)[1] == 0)
    start = jnp.broadcast_to(jnp.where(start, 1.0, 0.0)[:1], (tiles, tiles))
    local = jnp.broadcast_to(divide(line, halo_dev)[1].astype(jnp.float32)[:1], (tiles, tiles))
    down, across = iota((tiles, tiles), 0), iota((tiles, tiles), 1)
    before = (across <= down) & (divide(across, per)[0] == divide(down, per)[0])
    flat = jnp.concatenate([jnp.where(before, start, 0.0), jnp.where(across == down, local, 0.0)], axis=0)
    spread = lax.dot_general(
        flat.astype(jnp.bfloat16), jnp.ones((tiles, LANES), jnp.bfloat16), (((1,), (0,)), ((), ())),
        preferred_element_type=jnp.float32,
    )
    part, row = divide(spread[:tiles].astype(jnp.int32) - 1, sub)
    key = part * bin_dev + spread[tiles:].astype(jnp.int32)
    place_ref[...] = jnp.where(key == iota((tiles, LANES), 1), row, -1).astype(jnp.float32)

    one, zero = jnp.bfloat16(1), jnp.bfloat16(0)
    bin_ids = [
        (iota((PACK, LANES), 0) + k * PACK).astype(jnp.float32).astype(jnp.bfloat16) for k in range(bin_dev // PACK)
    ]
    field_id, range_id = divide(iota((lead, LANES), 0), rads)
    range_id = jnp.where(field_id < 3, range_id, -1)
    empty = jnp.zeros((2 * lead, LANES), jnp.bfloat16)

    for copy in copies[1:]:
        copy.wait()

    def one_group(group, acc_ref):
        acc_ref[...] = jnp.zeros_like(acc_ref)
        owner = owner_ref[halo_ref[group * per]]
        slot = jnp.int32(0)
        carry = None
        width = math.gcd(per, 2)
        for first in range(0, per, width):
            values, steps = [], []
            for k in range(first, first + width):
                t = group * per + k
                span, low = divide(bin_ref[pl.ds(t, 1), :], bin_dev)
                cells = pl.ds(pl.multiple_of(t * TILE, TILE), TILE)
                field = [jnp.broadcast_to(field_ref[f : f + 1, cells], (lead, LANES)) for f in range(3)]
                value = jnp.where(field_id == 0, field[0], jnp.where(field_id == 1, field[1], field[2]))
                value = jnp.where(jnp.broadcast_to(span, (lead, LANES)) == range_id, value, 0.0)
                high = value.astype(jnp.bfloat16)
                value = jnp.concatenate([high, (value - high.astype(jnp.float32)).astype(jnp.bfloat16)], axis=0)
                values.append(jnp.concatenate([empty] * (k - first) + [value] + [empty] * (first + width - 1 - k), axis=1))
                low = jnp.broadcast_to(low, (PACK, LANES)).astype(jnp.float32).astype(jnp.bfloat16)
                steps.append(jnp.concatenate([jnp.where(low <= ids, one, zero) for ids in bin_ids], axis=0))
            sums = matmul(jnp.concatenate(values, axis=0), jnp.concatenate(steps, axis=1), (1,))
            for k in range(first, first + width):
                at = (k - first) * 2 * lead
                tile_sum = sums[at : at + lead] + sums[at + lead : at + 2 * lead]
                if k:
                    fresh = halo_ref[group * per + k] != halo_ref[group * per + k - 1]
                    slot = slot + fresh.astype(jnp.int32)
                    carry = jnp.where(fresh, 0.0, carry) + tile_sum
                else:
                    carry = tile_sum
                acc_ref[pl.ds(pl.multiple_of(slot * lead, lead), lead), :bin_dev] = carry
        base = []
        side = lax.div(owner, spaces // 2)
        half = lax.div(lax.axis_index("space"), spaces // 2)
        for r in range(rads):
            place = lax.rem(owner, spaces // 2) * rads + jnp.where(side == half, r, r ^ 1)
            place = spaces // 2 * rads - 1 - place
            base.append((2 * place + side) * rows)
            places = jnp.max(place_ref[pl.ds(group * per, per), :], axis=0, keepdims=True)
            out_ref[pl.ds(base[r] + rows - 1, 1), :] = places
        for f in range(3):
            inner = [jnp.zeros((sub, bin_dev), jnp.float32)] * parts
            for r in range(rads):
                pieces = []
                for a in range(parts):
                    own = acc_ref[pl.ds(a * sub * lead + f * rads + r, sub, stride=lead), :][:, :bin_dev]
                    pieces.append(own + inner[a])
                    inner[a] = inner[a] + jnp.broadcast_to(own[:, bin_dev - 1 :], (sub, bin_dev))
                out_ref[pl.ds(base[r] + f * sub, sub), :] = jnp.concatenate(pieces, axis=1)

    unrolled = acc_ref.shape[0]
    for group in range(unrolled):
        one_group(group, acc_ref.at[group])

    @pl.loop(unrolled, tiles // per)
    def _(group):
        one_group(group, acc_ref.at[0])


def fold(x, height):
    return jnp.concatenate([x[k : k + height] for k in range(0, x.shape[0], height)], axis=1)


def merge_kernel(halo_dev, bin_dev, sub, rows, got_ref, own_ref, other_ref):
    sources = got_ref.shape[0] // (2 * rows)
    batch = math.gcd(sources, BATCH)
    row_ids = iota((sub, LANES), 0).astype(jnp.float32)

    def add(side, first):
        picks, values = [], []
        for i in range(batch):
            base = (2 * (first + i) + side) * rows
            places = jnp.broadcast_to(got_ref[pl.ds(base + rows - 1, 1), :], (sub, LANES))
            picks.append((places == row_ids).astype(jnp.float32))
            pieces = []
            for f in range(3):
                value = got_ref[pl.ds(base + f * sub, sub), :]
                high = value.astype(jnp.bfloat16).astype(jnp.float32)
                pieces.extend([high, value - high])
            values.append(jnp.concatenate(pieces, axis=1))
        pick = jnp.concatenate(picks, axis=0).astype(jnp.bfloat16)
        value = jnp.concatenate(values, axis=0).astype(jnp.bfloat16)
        return matmul(pick, value, (0,))

    results = []
    for side in range(2):
        sums = lax.fori_loop(
            1, sources // batch, lambda k, acc, side=side: acc + add(side, k * batch), add(side, 0)
        )
        fields = []
        for f in range(3):
            both = sums[:, 2 * f * LANES : (2 * f + 1) * LANES] + sums[:, (2 * f + 1) * LANES : (2 * f + 2) * LANES]
            acc = None
            for a in range(LANES // bin_dev):
                part = both[a * bin_dev : a * bin_dev + halo_dev, a * bin_dev : (a + 1) * bin_dev]
                acc = part if acc is None else acc + part
            fields.append(fold(acc, halo_dev // (LANES // bin_dev)))
        results.append(jnp.concatenate(fields, axis=0))
    first = lax.axis_index("space") < lax.axis_size("space") // 2
    own_ref[...] = jnp.where(first, results[0], results[1])
    other_ref[...] = jnp.where(first, results[1], results[0])


def finish_kernel(halo_dev, bin_dev, own_ref, got_ref, mass_ref, volume_ref, entropy_ref, speed_ref):
    total = own_ref[...] + got_ref[...]
    height = halo_dev * bin_dev // LANES
    total = [
        jnp.concatenate(
            [total[f * height : (f + 1) * height, a : a + bin_dev] for a in range(0, LANES, bin_dev)], axis=0
        )
        for f in range(3)
    ]
    mass_ref[...], volume_ref[...], entropy_ref[...] = total
    first = lax.axis_index("rad") * bin_dev + 1
    position = (iota((1, bin_dev), 1) + first).astype(jnp.float32)
    radius = jnp.exp(log_inner + position * (-log_inner / BINS))
    speed_ref[...] = jnp.sqrt(total[0] / radius)


def body(cell_bin, cell_fields, tile_halo, halo_owner):
    spaces = lax.axis_size("space")
    rads = lax.axis_size("rad")
    bin_dev = BINS // rads
    tiles = tile_halo.shape[0]
    halo_dev = halo_owner.shape[0] // spaces
    per = max(2, 2 * tiles // spaces)
    slots = -(-max(1, per // 2) // PACK) * PACK
    sub = slots * bin_dev // LANES
    rows = 3 * sub + 1
    devices = spaces * rads
    vmem = pl.BlockSpec(memory_space=pltpu.VMEM)
    hbm = pl.BlockSpec(memory_space=pltpu.HBM)
    params = pltpu.CompilerParams(vmem_limit_bytes=VMEM_LIMIT)
    outgoing = pl.pallas_call(
        functools.partial(bin_kernel, spaces, rads, per, slots, rows),
        out_shape=jax.ShapeDtypeStruct((devices * rows, LANES), jnp.float32),
        in_specs=[hbm] * 5,
        out_specs=vmem,
        scratch_shapes=[
            pltpu.SMEM(halo_owner.shape, jnp.int32),
            pltpu.SMEM((tiles,), jnp.int32),
            pltpu.VMEM((1, tiles), jnp.int32),
            pltpu.VMEM((tiles, TILE), jnp.int32),
            pltpu.VMEM(cell_fields.shape, jnp.float32),
            pltpu.VMEM((tiles, LANES), jnp.float32),
            pltpu.VMEM((min(UNROLL, tiles // per), slots * FIELDS * rads, LANES), jnp.float32),
            pltpu.SemaphoreType.DMA((5,)),
        ],
        compiler_params=params,
    )(
        *[
            pltpu.with_memory_space_constraint(x, pltpu.HBM)
            for x in (halo_owner, tile_halo, tile_halo.reshape(1, tiles), cell_bin.reshape(tiles, TILE), cell_fields)
        ]
    )
    order = range(devices // 2 - 1, -1, -1)
    received = lax.all_to_all(
        outgoing.reshape(devices // 2, 2 * rows, 1, LANES),
        ("space", "rad"),
        split_axis=0,
        concat_axis=0,
        axis_index_groups=[[side * (devices // 2) + k for k in order] for side in range(2)],
        tiled=True,
    )
    own, other = pl.pallas_call(
        functools.partial(merge_kernel, halo_dev, bin_dev, sub, rows),
        out_shape=[jax.ShapeDtypeStruct((3 * halo_dev * bin_dev // LANES, LANES), jnp.float32)] * 2,
        in_specs=[vmem],
        out_specs=[vmem] * 2,
        compiler_params=params,
    )(received.reshape(devices * rows, LANES))
    partners = [(d, (d + devices // 2) % devices ^ 1) for d in range(devices)]
    got = lax.ppermute(other, ("space", "rad"), partners)
    return pl.pallas_call(
        functools.partial(finish_kernel, halo_dev, bin_dev),
        out_shape=[jax.ShapeDtypeStruct((halo_dev, bin_dev), jnp.float32)] * 4,
        in_specs=[vmem] * 2,
        out_specs=[vmem] * 4,
        compiler_params=params,
    )(own, got)


def solution(mesh):
    in_specs = (P(("space", "rad")), P(None, ("space", "rad")), P(("space", "rad")), P())
    out_specs = (P("space", "rad"), P("space", "rad"), P("space", "rad"), P("space", "rad"))
    return jax.shard_map(body, mesh=mesh, in_specs=in_specs, out_specs=out_specs, check_vma=False)
```

```python
import functools
import math

import jax
import jax.numpy as jnp
from jax import lax
from jax.experimental import pallas as pl
from jax.experimental.pallas import tpu as pltpu
from jax.sharding import PartitionSpec as P

TILE = 128
BINS = 256
LANES = 128
PACK = 16
FIELDS = 4
UNROLL = 4
BATCH = 32
VMEM_LIMIT = 16 * 1024 * 1024

log_inner = -2.302585092994046


def divide(x, n):
    if n & (n - 1):
        return lax.div(x, jnp.full_like(x, n)), lax.rem(x, jnp.full_like(x, n))
    return lax.shift_right_logical(x, jnp.full_like(x, n.bit_length() - 1)), x & (n - 1)


def iota(shape, dim):
    return lax.broadcasted_iota(jnp.int32, shape, dim)


def matmul(a, b, contract):
    return lax.dot_general(a, b, ((contract, contract), ((), ())), preferred_element_type=jnp.float32)


def bin_kernel(
    spaces, rads, per, slots, rows,
    owner_hbm, halo_hbm, line_hbm, bin_hbm, field_hbm, out_ref,
    owner_ref, halo_ref, line_ref, bin_ref, span_ref, low_ref, field_ref, place_ref, acc_ref, sem,
):
    tiles = bin_ref.shape[0]
    halo_dev = owner_ref.shape[0] // spaces
    bin_dev = BINS // rads
    parts = LANES // bin_dev
    sub = slots // parts
    lead = FIELDS * rads
    copies = [
        pltpu.make_async_copy(source, target, sem.at[k])
        for k, (source, target) in enumerate(
            [(line_hbm, line_ref), (halo_hbm, halo_ref), (owner_hbm, owner_ref), (bin_hbm, bin_ref), (field_hbm, field_ref)]
        )
    ]
    for copy in copies:
        copy.start()

    @pl.loop(0, spaces * rads)
    def _(block):
        out_ref[pl.ds(block * rows, rows - 1), :] = jnp.zeros((rows - 1, LANES), jnp.float32)
        out_ref[pl.ds(block * rows + rows - 1, 1), :] = jnp.full((1, LANES), -1.0, jnp.float32)

    for copy in copies[:1]:
        copy.wait()
    line = jnp.broadcast_to(line_ref[...], (8, tiles))
    start = (line != pltpu.roll(line, 1, 1)) | (divide(iota((8, tiles), 1), per)[1] == 0)
    start = jnp.broadcast_to(jnp.where(start, 1.0, 0.0)[:1], (tiles, tiles))
    local = jnp.broadcast_to(divide(line, halo_dev)[1].astype(jnp.float32)[:1], (tiles, tiles))
    down, across = iota((tiles, tiles), 0), iota((tiles, tiles), 1)
    before = (across <= down) & (divide(across, per)[0] == divide(down, per)[0])
    flat = jnp.concatenate([jnp.where(before, start, 0.0), jnp.where(across == down, local, 0.0)], axis=0)
    spread = lax.dot_general(
        flat.astype(jnp.bfloat16), jnp.ones((tiles, LANES), jnp.bfloat16), (((1,), (0,)), ((), ())),
        preferred_element_type=jnp.float32,
    )
    part, row = divide(spread[:tiles].astype(jnp.int32) - 1, sub)
    key = part * halo_dev + spread[tiles:].astype(jnp.int32)
    place_ref[...] = jnp.where(key == iota((tiles, LANES), 1), row, -1).astype(jnp.float32)

    one, zero = jnp.bfloat16(1), jnp.bfloat16(0)
    bin_ids = [
        (iota((PACK, LANES), 0) + k * PACK).astype(jnp.float32).astype(jnp.bfloat16) for k in range(bin_dev // PACK)
    ]
    field_id, range_id = divide(iota((2 * rads, LANES), 0), rads)
    empty = jnp.zeros((2 * lead, LANES), jnp.bfloat16)

    for copy in copies[1:]:
        copy.wait()
    span_ref[...], low = divide(bin_ref[...], bin_dev)
    low_ref[...] = low.astype(jnp.float32)

    def one_group(group, acc_ref):
        acc_ref[...] = jnp.zeros_like(acc_ref)
        owner = owner_ref[halo_ref[group * per]]
        slot = jnp.int32(0)
        carry = None
        width = math.gcd(per, 2)
        for first in range(0, per, width):
            values, steps = [], []
            for k in range(first, first + width):
                t = group * per + k
                span, low = span_ref[pl.ds(t, 1), :], low_ref[pl.ds(t, 1), :]
                cells = pl.ds(pl.multiple_of(t * TILE, TILE), TILE)
                field = [jnp.broadcast_to(field_ref[f : f + 1, cells], (2 * rads, LANES)) for f in range(3)]
                inside = jnp.broadcast_to(span, (2 * rads, LANES)) == range_id
                value = [jnp.where(field_id == 0, field[0], field[1]), field[2]]
                value = jnp.concatenate([jnp.where(inside, v, 0.0) for v in value], axis=0)
                high = value.astype(jnp.bfloat16)
                value = jnp.concatenate([high, (value - high.astype(jnp.float32)).astype(jnp.bfloat16)], axis=0)
                values.append(jnp.concatenate([empty] * (k - first) + [value] + [empty] * (first + width - 1 - k), axis=1))
                low = jnp.broadcast_to(low, (PACK, LANES)).astype(jnp.bfloat16)
                steps.append(jnp.concatenate([jnp.where(low <= ids, one, zero) for ids in bin_ids], axis=0))
            sums = matmul(jnp.concatenate(values, axis=0), jnp.concatenate(steps, axis=1), (1,))
            for k in range(first, first + width):
                at = (k - first) * 2 * lead
                tile_sum = sums[at : at + lead] + sums[at + lead : at + 2 * lead]
                if k:
                    fresh = halo_ref[group * per + k] != halo_ref[group * per + k - 1]
                    slot = slot + fresh.astype(jnp.int32)
                    carry = jnp.where(fresh, 0.0, carry) + tile_sum
                else:
                    carry = tile_sum
                acc_ref[pl.ds(pl.multiple_of(slot * lead, lead), lead), :bin_dev] = carry
        base = []
        side = lax.div(owner, spaces // 2)
        half = lax.div(lax.axis_index("space"), spaces // 2)
        for r in range(rads):
            place = lax.rem(owner, spaces // 2) * rads + jnp.where(side == half, r, r ^ 1)
            place = spaces // 2 * rads - 1 - place
            base.append((2 * place + side) * rows)
            places = jnp.max(place_ref[pl.ds(group * per, per), :], axis=0, keepdims=True)
            out_ref[pl.ds(base[r] + rows - 1, 1), :] = places
        for f in range(3):
            inner = [jnp.zeros((sub, bin_dev), jnp.float32)] * parts
            for r in range(rads):
                pieces = []
                for a in range(parts):
                    own = acc_ref[pl.ds(a * sub * lead + f * rads + r, sub, stride=lead), :][:, :bin_dev]
                    pieces.append(own + inner[a])
                    inner[a] = inner[a] + jnp.broadcast_to(own[:, bin_dev - 1 :], (sub, bin_dev))
                out_ref[pl.ds(base[r] + f * sub, sub), :] = jnp.concatenate(pieces, axis=1)

    unrolled = acc_ref.shape[0]
    for group in range(unrolled):
        one_group(group, acc_ref.at[group])

    @pl.loop(unrolled, tiles // per)
    def _(group):
        one_group(group, acc_ref.at[0])


def fold(x, height):
    return jnp.concatenate([x[k : k + height] for k in range(0, x.shape[0], height)], axis=1)


def merge_kernel(halo_dev, bin_dev, sub, rows, got_ref, own_ref, other_ref):
    sources = got_ref.shape[0] // (2 * rows)
    batch = math.gcd(sources, BATCH)
    parts = LANES // bin_dev
    row_ids = iota((sub, LANES), 0).astype(jnp.float32)

    def add(side, first):
        picks, values = [], []
        for i in range(batch):
            base = (2 * (first + i) + side) * rows
            places = jnp.broadcast_to(got_ref[pl.ds(base + rows - 1, 1), :], (sub, LANES))
            picks.append((places == row_ids).astype(jnp.float32)[:, : parts * halo_dev])
            pieces = []
            for f in range(3):
                value = got_ref[pl.ds(base + f * sub, sub), :]
                high = value.astype(jnp.bfloat16).astype(jnp.float32)
                pieces.extend([high, value - high])
            values.append(jnp.concatenate(pieces, axis=1))
        pick = jnp.concatenate(picks, axis=0).astype(jnp.bfloat16)
        value = jnp.concatenate(values, axis=0).astype(jnp.bfloat16)
        return matmul(pick, value, (0,))

    results = []
    for side in range(2):
        sums = lax.fori_loop(
            1, sources // batch, lambda k, acc, side=side: acc + add(side, k * batch), add(side, 0)
        )
        fields = []
        for f in range(3):
            both = sums[:, 2 * f * LANES : (2 * f + 1) * LANES] + sums[:, (2 * f + 1) * LANES : (2 * f + 2) * LANES]
            acc = None
            for a in range(parts):
                part = both[a * halo_dev : (a + 1) * halo_dev, a * bin_dev : (a + 1) * bin_dev]
                acc = part if acc is None else acc + part
            fields.append(fold(acc, halo_dev // (LANES // bin_dev)))
        results.append(jnp.concatenate(fields, axis=0))
    first = lax.axis_index("space") < lax.axis_size("space") // 2
    own_ref[...] = jnp.where(first, results[0], results[1])
    other_ref[...] = jnp.where(first, results[1], results[0])


def finish_kernel(halo_dev, bin_dev, own_ref, got_ref, mass_ref, volume_ref, entropy_ref, speed_ref):
    total = own_ref[...] + got_ref[...]
    height = halo_dev * bin_dev // LANES
    total = [
        jnp.concatenate(
            [total[f * height : (f + 1) * height, a : a + bin_dev] for a in range(0, LANES, bin_dev)], axis=0
        )
        for f in range(3)
    ]
    mass_ref[...], volume_ref[...], entropy_ref[...] = total
    first = lax.axis_index("rad") * bin_dev + 1
    position = (iota((1, bin_dev), 1) + first).astype(jnp.float32)
    radius = jnp.exp(log_inner + position * (-log_inner / BINS))
    speed_ref[...] = jnp.sqrt(total[0] / radius)


def body(cell_bin, cell_fields, tile_halo, halo_owner):
    spaces = lax.axis_size("space")
    rads = lax.axis_size("rad")
    bin_dev = BINS // rads
    tiles = tile_halo.shape[0]
    halo_dev = halo_owner.shape[0] // spaces
    per = max(2, 2 * tiles // spaces)
    slots = -(-max(1, per // 2) // PACK) * PACK
    sub = slots * bin_dev // LANES
    rows = 3 * sub + 1
    devices = spaces * rads
    vmem = pl.BlockSpec(memory_space=pltpu.VMEM)
    hbm = pl.BlockSpec(memory_space=pltpu.HBM)
    params = pltpu.CompilerParams(vmem_limit_bytes=VMEM_LIMIT)
    outgoing = pl.pallas_call(
        functools.partial(bin_kernel, spaces, rads, per, slots, rows),
        out_shape=jax.ShapeDtypeStruct((devices * rows, LANES), jnp.float32),
        in_specs=[hbm] * 5,
        out_specs=vmem,
        scratch_shapes=[
            pltpu.SMEM(halo_owner.shape, jnp.int32),
            pltpu.SMEM((tiles,), jnp.int32),
            pltpu.VMEM((1, tiles), jnp.int32),
            pltpu.VMEM((tiles, TILE), jnp.int32),
            pltpu.VMEM((tiles, TILE), jnp.int32),
            pltpu.VMEM((tiles, TILE), jnp.float32),
            pltpu.VMEM(cell_fields.shape, jnp.float32),
            pltpu.VMEM((tiles, LANES), jnp.float32),
            pltpu.VMEM((min(UNROLL, tiles // per), slots * FIELDS * rads, LANES), jnp.float32),
            pltpu.SemaphoreType.DMA((5,)),
        ],
        compiler_params=params,
    )(
        *[
            pltpu.with_memory_space_constraint(x, pltpu.HBM)
            for x in (halo_owner, tile_halo, tile_halo.reshape(1, tiles), cell_bin.reshape(tiles, TILE), cell_fields)
        ]
    )
    order = range(devices // 2 - 1, -1, -1)
    received = lax.all_to_all(
        outgoing.reshape(devices // 2, 2 * rows, 1, LANES),
        ("space", "rad"),
        split_axis=0,
        concat_axis=0,
        axis_index_groups=[[side * (devices // 2) + k for k in order] for side in range(2)],
        tiled=True,
    )
    own, other = pl.pallas_call(
        functools.partial(merge_kernel, halo_dev, bin_dev, sub, rows),
        out_shape=[jax.ShapeDtypeStruct((3 * halo_dev * bin_dev // LANES, LANES), jnp.float32)] * 2,
        in_specs=[vmem],
        out_specs=[vmem] * 2,
        compiler_params=params,
    )(received.reshape(devices * rows, LANES))
    partners = [(d, (d + devices // 2) % devices ^ 1) for d in range(devices)]
    got = lax.ppermute(other, ("space", "rad"), partners)
    return pl.pallas_call(
        functools.partial(finish_kernel, halo_dev, bin_dev),
        out_shape=[jax.ShapeDtypeStruct((halo_dev, bin_dev), jnp.float32)] * 4,
        in_specs=[vmem] * 2,
        out_specs=[vmem] * 4,
        compiler_params=params,
    )(own, got)


def solution(mesh):
    in_specs = (P(("space", "rad")), P(None, ("space", "rad")), P(("space", "rad")), P())
    out_specs = (P("space", "rad"), P("space", "rad"), P("space", "rad"), P("space", "rad"))
    return jax.shard_map(body, mesh=mesh, in_specs=in_specs, out_specs=out_specs, check_vma=False)
```

```python
import functools
import math

import jax
import jax.numpy as jnp
from jax import lax
from jax.experimental import pallas as pl
from jax.experimental.pallas import tpu as pltpu
from jax.sharding import PartitionSpec as P

TILE = 128
BINS = 256
LANES = 128
PACK = 16
FIELDS = 4
UNROLL = 4
MERGE_FLOPS = 10**7
BATCH = 32
VMEM_LIMIT = 16 * 1024 * 1024

log_inner = -2.302585092994046


def divide(x, n):
    if n & (n - 1):
        return lax.div(x, jnp.full_like(x, n)), lax.rem(x, jnp.full_like(x, n))
    return lax.shift_right_logical(x, jnp.full_like(x, n.bit_length() - 1)), x & (n - 1)


def iota(shape, dim):
    return lax.broadcasted_iota(jnp.int32, shape, dim)


def matmul(a, b, contract):
    return lax.dot_general(a, b, ((contract, contract), ((), ())), preferred_element_type=jnp.float32)


def bin_kernel(
    spaces, rads, per, slots, rows,
    owner_hbm, halo_hbm, line_hbm, bin_hbm, field_hbm, out_ref,
    owner_ref, halo_ref, line_ref, bin_ref, span_ref, low_ref, field_ref, place_ref, acc_ref, sem,
):
    tiles = bin_ref.shape[0]
    halo_dev = owner_ref.shape[0] // spaces
    bin_dev = BINS // rads
    parts = LANES // bin_dev
    sub = slots // parts
    lead = FIELDS * rads
    copies = [
        pltpu.make_async_copy(source, target, sem.at[k])
        for k, (source, target) in enumerate(
            [(line_hbm, line_ref), (halo_hbm, halo_ref), (owner_hbm, owner_ref), (bin_hbm, bin_ref), (field_hbm, field_ref)]
        )
    ]
    for copy in copies:
        copy.start()

    @pl.loop(0, spaces * rads)
    def _(block):
        out_ref[pl.ds(block * rows, rows - 1), :] = jnp.zeros((rows - 1, LANES), jnp.float32)
        out_ref[pl.ds(block * rows + rows - 1, 1), :] = jnp.full((1, LANES), -1.0, jnp.float32)

    for copy in copies[:1]:
        copy.wait()
    line = jnp.broadcast_to(line_ref[...], (8, tiles))
    start = (line != pltpu.roll(line, 1, 1)) | (divide(iota((8, tiles), 1), per)[1] == 0)
    start = jnp.broadcast_to(jnp.where(start, 1.0, 0.0)[:1], (tiles, tiles))
    local = jnp.broadcast_to(divide(line, halo_dev)[1].astype(jnp.float32)[:1], (tiles, tiles))
    down, across = iota((tiles, tiles), 0), iota((tiles, tiles), 1)
    before = (across <= down) & (divide(across, per)[0] == divide(down, per)[0])
    flat = jnp.concatenate([jnp.where(before, start, 0.0), jnp.where(across == down, local, 0.0)], axis=0)
    spread = lax.dot_general(
        flat.astype(jnp.bfloat16), jnp.ones((tiles, LANES), jnp.bfloat16), (((1,), (0,)), ((), ())),
        preferred_element_type=jnp.float32,
    )
    part, row = divide(spread[:tiles].astype(jnp.int32) - 1, sub)
    key = part * halo_dev + spread[tiles:].astype(jnp.int32)
    place_ref[...] = jnp.where(key == iota((tiles, LANES), 1), row, -1).astype(jnp.float32)

    one, zero = jnp.bfloat16(1), jnp.bfloat16(0)
    bin_ids = [
        (iota((PACK, LANES), 0) + k * PACK).astype(jnp.float32).astype(jnp.bfloat16) for k in range(bin_dev // PACK)
    ]
    field_id, range_id = divide(iota((2 * rads, LANES), 0), rads)
    empty = jnp.zeros((2 * lead, LANES), jnp.bfloat16)

    for copy in copies[1:]:
        copy.wait()
    span_ref[...], low = divide(bin_ref[...], bin_dev)
    low_ref[...] = low.astype(jnp.float32)

    def one_group(group, acc_ref):
        acc_ref[...] = jnp.zeros_like(acc_ref)
        owner = owner_ref[halo_ref[group * per]]
        slot = jnp.int32(0)
        carry = None
        width = math.gcd(per, 2)
        for first in range(0, per, width):
            values, steps = [], []
            for k in range(first, first + width):
                t = group * per + k
                span, low = span_ref[pl.ds(t, 1), :], low_ref[pl.ds(t, 1), :]
                cells = pl.ds(pl.multiple_of(t * TILE, TILE), TILE)
                field = [jnp.broadcast_to(field_ref[f : f + 1, cells], (2 * rads, LANES)) for f in range(3)]
                inside = jnp.broadcast_to(span, (2 * rads, LANES)) == range_id
                value = [jnp.where(field_id == 0, field[0], field[1]), field[2]]
                value = jnp.concatenate([jnp.where(inside, v, 0.0) for v in value], axis=0)
                high = value.astype(jnp.bfloat16)
                value = jnp.concatenate([high, (value - high.astype(jnp.float32)).astype(jnp.bfloat16)], axis=0)
                values.append(jnp.concatenate([empty] * (k - first) + [value] + [empty] * (first + width - 1 - k), axis=1))
                low = jnp.broadcast_to(low, (PACK, LANES)).astype(jnp.bfloat16)
                steps.append(jnp.concatenate([jnp.where(low <= ids, one, zero) for ids in bin_ids], axis=0))
            sums = matmul(jnp.concatenate(values, axis=0), jnp.concatenate(steps, axis=1), (1,))
            for k in range(first, first + width):
                at = (k - first) * 2 * lead
                tile_sum = sums[at : at + lead] + sums[at + lead : at + 2 * lead]
                if k:
                    fresh = halo_ref[group * per + k] != halo_ref[group * per + k - 1]
                    slot = slot + fresh.astype(jnp.int32)
                    carry = jnp.where(fresh, 0.0, carry) + tile_sum
                else:
                    carry = tile_sum
                acc_ref[pl.ds(pl.multiple_of(slot * lead, lead), lead), :bin_dev] = carry
        base = []
        side = lax.div(owner, spaces // 2)
        half = lax.div(lax.axis_index("space"), spaces // 2)
        for r in range(rads):
            place = lax.rem(owner, spaces // 2) * rads + jnp.where(side == half, r, r ^ 1)
            place = spaces // 2 * rads - 1 - place
            base.append((2 * place + side) * rows)
            places = jnp.max(place_ref[pl.ds(group * per, per), :], axis=0, keepdims=True)
            out_ref[pl.ds(base[r] + rows - 1, 1), :] = places
        for f in range(3):
            inner = [jnp.zeros((sub, bin_dev), jnp.float32)] * parts
            for r in range(rads):
                pieces = []
                for a in range(parts):
                    own = acc_ref[pl.ds(a * sub * lead + f * rads + r, sub, stride=lead), :][:, :bin_dev]
                    pieces.append(own + inner[a])
                    inner[a] = inner[a] + jnp.broadcast_to(own[:, bin_dev - 1 :], (sub, bin_dev))
                out_ref[pl.ds(base[r] + f * sub, sub), :] = jnp.concatenate(pieces, axis=1)

    unrolled = acc_ref.shape[0]
    for group in range(unrolled):
        one_group(group, acc_ref.at[group])

    @pl.loop(unrolled, tiles // per)
    def _(group):
        one_group(group, acc_ref.at[0])


def fold(x, height):
    return jnp.concatenate([x[k : k + height] for k in range(0, x.shape[0], height)], axis=1)


def merge_kernel(mine, halo_dev, bin_dev, sub, rows, got_ref, sum_ref):
    sources = got_ref.shape[0] // (2 * rows)
    batch = math.gcd(sources, BATCH)
    parts = LANES // bin_dev
    row_ids = iota((sub, LANES), 0).astype(jnp.float32)
    half = lax.div(lax.axis_index("space"), lax.axis_size("space") // 2)
    side = half if mine else 1 - half

    def add(first):
        picks, values = [], []
        for i in range(batch):
            base = (2 * (first + i) + side) * rows
            places = jnp.broadcast_to(got_ref[pl.ds(base + rows - 1, 1), :], (sub, LANES))
            picks.append((places == row_ids).astype(jnp.float32)[:, : parts * halo_dev])
            pieces = []
            for f in range(3):
                value = got_ref[pl.ds(base + f * sub, sub), :]
                high = value.astype(jnp.bfloat16).astype(jnp.float32)
                pieces.extend([high, value - high])
            values.append(jnp.concatenate(pieces, axis=1))
        pick = jnp.concatenate(picks, axis=0).astype(jnp.bfloat16)
        value = jnp.concatenate(values, axis=0).astype(jnp.bfloat16)
        return matmul(pick, value, (0,))

    sums = lax.fori_loop(1, sources // batch, lambda k, acc: acc + add(k * batch), add(0))
    fields = []
    for f in range(3):
        both = sums[:, 2 * f * LANES : (2 * f + 1) * LANES] + sums[:, (2 * f + 1) * LANES : (2 * f + 2) * LANES]
        acc = None
        for a in range(parts):
            part = both[a * halo_dev : (a + 1) * halo_dev, a * bin_dev : (a + 1) * bin_dev]
            acc = part if acc is None else acc + part
        fields.append(fold(acc, halo_dev // (LANES // bin_dev)))
    sum_ref[...] = jnp.concatenate(fields, axis=0)


def finish_kernel(halo_dev, bin_dev, own_ref, got_ref, mass_ref, volume_ref, entropy_ref, speed_ref):
    total = own_ref[...] + got_ref[...]
    height = halo_dev * bin_dev // LANES
    total = [
        jnp.concatenate(
            [total[f * height : (f + 1) * height, a : a + bin_dev] for a in range(0, LANES, bin_dev)], axis=0
        )
        for f in range(3)
    ]
    mass_ref[...], volume_ref[...], entropy_ref[...] = total
    first = lax.axis_index("rad") * bin_dev + 1
    position = (iota((1, bin_dev), 1) + first).astype(jnp.float32)
    radius = jnp.exp(log_inner + position * (-log_inner / BINS))
    speed_ref[...] = jnp.sqrt(total[0] / radius)


def body(cell_bin, cell_fields, tile_halo, halo_owner):
    spaces = lax.axis_size("space")
    rads = lax.axis_size("rad")
    bin_dev = BINS // rads
    tiles = tile_halo.shape[0]
    halo_dev = halo_owner.shape[0] // spaces
    per = max(2, 2 * tiles // spaces)
    slots = -(-max(1, per // 2) // PACK) * PACK
    sub = slots * bin_dev // LANES
    rows = 3 * sub + 1
    devices = spaces * rads
    vmem = pl.BlockSpec(memory_space=pltpu.VMEM)
    hbm = pl.BlockSpec(memory_space=pltpu.HBM)
    params = pltpu.CompilerParams(vmem_limit_bytes=VMEM_LIMIT)
    outgoing = pl.pallas_call(
        functools.partial(bin_kernel, spaces, rads, per, slots, rows),
        out_shape=jax.ShapeDtypeStruct((devices * rows, LANES), jnp.float32),
        in_specs=[hbm] * 5,
        out_specs=vmem,
        scratch_shapes=[
            pltpu.SMEM(halo_owner.shape, jnp.int32),
            pltpu.SMEM((tiles,), jnp.int32),
            pltpu.VMEM((1, tiles), jnp.int32),
            pltpu.VMEM((tiles, TILE), jnp.int32),
            pltpu.VMEM((tiles, TILE), jnp.int32),
            pltpu.VMEM((tiles, TILE), jnp.float32),
            pltpu.VMEM(cell_fields.shape, jnp.float32),
            pltpu.VMEM((tiles, LANES), jnp.float32),
            pltpu.VMEM((min(UNROLL, tiles // per), slots * FIELDS * rads, LANES), jnp.float32),
            pltpu.SemaphoreType.DMA((5,)),
        ],
        compiler_params=pltpu.CompilerParams(
            vmem_limit_bytes=VMEM_LIMIT
        ),
    )(
        *[
            pltpu.with_memory_space_constraint(x, pltpu.HBM)
            for x in (halo_owner, tile_halo, tile_halo.reshape(1, tiles), cell_bin.reshape(tiles, TILE), cell_fields)
        ]
    )
    order = range(devices // 2 - 1, -1, -1)
    received = lax.all_to_all(
        outgoing.reshape(devices // 2, 2 * rows, 1, LANES),
        ("space", "rad"),
        split_axis=0,
        concat_axis=0,
        axis_index_groups=[[side * (devices // 2) + k for k in order] for side in range(2)],
        tiled=True,
    )
    received = received.reshape(devices * rows, LANES)
    own, other = (
        pl.pallas_call(
            functools.partial(merge_kernel, mine, halo_dev, bin_dev, sub, rows),
            out_shape=jax.ShapeDtypeStruct((3 * halo_dev * bin_dev // LANES, LANES), jnp.float32),
            in_specs=[vmem],
            out_specs=vmem,
            compiler_params=params,
            cost_estimate=pl.CostEstimate(flops=MERGE_FLOPS, bytes_accessed=devices * rows * LANES * 2, transcendentals=0),
        )(received)
        for mine in (True, False)
    )
    partners = [(d, (d + devices // 2) % devices ^ 1) for d in range(devices)]
    got = lax.ppermute(other, ("space", "rad"), partners)
    return pl.pallas_call(
        functools.partial(finish_kernel, halo_dev, bin_dev),
        out_shape=[jax.ShapeDtypeStruct((halo_dev, bin_dev), jnp.float32)] * 4,
        in_specs=[vmem] * 2,
        out_specs=[vmem] * 4,
        compiler_params=params,
    )(own, got)


def solution(mesh):
    in_specs = (P(("space", "rad")), P(None, ("space", "rad")), P(("space", "rad")), P())
    out_specs = (P("space", "rad"), P("space", "rad"), P("space", "rad"), P("space", "rad"))
    return jax.shard_map(body, mesh=mesh, in_specs=in_specs, out_specs=out_specs, check_vma=False)
```

```python
import functools
import math

import jax
import jax.numpy as jnp
from jax import lax
from jax.experimental import pallas as pl
from jax.experimental.pallas import tpu as pltpu
from jax.sharding import PartitionSpec as P

TILE = 128
BINS = 256
LANES = 128
PACK = 16
FIELDS = 4
UNROLL = 4
MERGE_FLOPS = 10**7
BATCH = 32
VMEM_LIMIT = 16 * 1024 * 1024

log_inner = -2.302585092994046


def divide(x, n):
    if n & (n - 1):
        return lax.div(x, jnp.full_like(x, n)), lax.rem(x, jnp.full_like(x, n))
    return lax.shift_right_logical(x, jnp.full_like(x, n.bit_length() - 1)), x & (n - 1)


def iota(shape, dim):
    return lax.broadcasted_iota(jnp.int32, shape, dim)


def matmul(a, b, contract):
    return lax.dot_general(a, b, ((contract, contract), ((), ())), preferred_element_type=jnp.float32)


def bin_kernel(
    spaces, rads, per, slots, rows,
    owner_hbm, halo_hbm, line_hbm, bin_hbm, field_hbm, out_ref,
    owner_ref, halo_ref, line_ref, bin_ref, span_ref, low_ref, field_ref, place_ref, acc_ref, sem,
):
    tiles = bin_ref.shape[0]
    halo_dev = owner_ref.shape[0] // spaces
    bin_dev = BINS // rads
    parts = LANES // bin_dev
    sub = slots // parts
    lead = FIELDS * rads
    copies = [
        pltpu.make_async_copy(source, target, sem.at[k])
        for k, (source, target) in enumerate(
            [(line_hbm, line_ref), (halo_hbm, halo_ref), (owner_hbm, owner_ref), (bin_hbm, bin_ref), (field_hbm, field_ref)]
        )
    ]
    for copy in copies:
        copy.start()

    @pl.loop(0, spaces * rads)
    def _(block):
        out_ref[pl.ds(block * rows, rows - 1), :] = jnp.zeros((rows - 1, LANES), jnp.float32)
        out_ref[pl.ds(block * rows + rows - 1, 1), :] = jnp.full((1, LANES), -1.0, jnp.float32)

    for copy in copies[:1]:
        copy.wait()
    line = jnp.broadcast_to(line_ref[...], (8, tiles))
    start = (line != pltpu.roll(line, 1, 1)) | (divide(iota((8, tiles), 1), per)[1] == 0)
    start = jnp.broadcast_to(jnp.where(start, 1.0, 0.0)[:1], (tiles, tiles))
    local = jnp.broadcast_to(divide(line, halo_dev)[1].astype(jnp.float32)[:1], (tiles, tiles))
    down, across = iota((tiles, tiles), 0), iota((tiles, tiles), 1)
    before = (across <= down) & (divide(across, per)[0] == divide(down, per)[0])
    flat = jnp.concatenate([jnp.where(before, start, 0.0), jnp.where(across == down, local, 0.0)], axis=0)
    spread = lax.dot_general(
        flat.astype(jnp.bfloat16), jnp.ones((tiles, LANES), jnp.bfloat16), (((1,), (0,)), ((), ())),
        preferred_element_type=jnp.float32,
    )
    part, row = divide(spread[:tiles].astype(jnp.int32) - 1, sub)
    key = part * halo_dev + spread[tiles:].astype(jnp.int32)
    place_ref[...] = jnp.where(key == iota((tiles, LANES), 1), row, -1).astype(jnp.float32)

    one, zero = jnp.bfloat16(1), jnp.bfloat16(0)
    bin_ids = [
        (iota((PACK, LANES), 0) + k * PACK).astype(jnp.float32).astype(jnp.bfloat16) for k in range(bin_dev // PACK)
    ]
    field_id, range_id = divide(iota((2 * rads, LANES), 0), rads)
    empty = jnp.zeros((2 * lead, LANES), jnp.bfloat16)

    for copy in copies[1:]:
        copy.wait()
    span_ref[...], low = divide(bin_ref[...], bin_dev)
    low_ref[...] = low.astype(jnp.float32)

    def one_group(group, acc_ref):
        acc_ref[...] = jnp.zeros_like(acc_ref)
        owner = owner_ref[halo_ref[group * per]]
        slot = jnp.int32(0)
        carry = None
        width = math.gcd(per, 2)
        for first in range(0, per, width):
            values, steps = [], []
            for k in range(first, first + width):
                t = group * per + k
                span, low = span_ref[pl.ds(t, 1), :], low_ref[pl.ds(t, 1), :]
                cells = pl.ds(pl.multiple_of(t * TILE, TILE), TILE)
                field = [jnp.broadcast_to(field_ref[f : f + 1, cells], (2 * rads, LANES)) for f in range(3)]
                inside = jnp.broadcast_to(span, (2 * rads, LANES)) == range_id
                value = [jnp.where(field_id == 0, field[0], field[1]), field[2]]
                value = jnp.concatenate([jnp.where(inside, v, 0.0) for v in value], axis=0)
                high = value.astype(jnp.bfloat16)
                value = jnp.concatenate([high, (value - high.astype(jnp.float32)).astype(jnp.bfloat16)], axis=0)
                values.append(jnp.concatenate([empty] * (k - first) + [value] + [empty] * (first + width - 1 - k), axis=1))
                low = jnp.broadcast_to(low, (PACK, LANES)).astype(jnp.bfloat16)
                steps.append(jnp.concatenate([jnp.where(low <= ids, one, zero) for ids in bin_ids], axis=0))
            sums = matmul(jnp.concatenate(values, axis=0), jnp.concatenate(steps, axis=1), (1,))
            for k in range(first, first + width):
                at = (k - first) * 2 * lead
                tile_sum = sums[at : at + lead] + sums[at + lead : at + 2 * lead]
                if k:
                    fresh = halo_ref[group * per + k] != halo_ref[group * per + k - 1]
                    slot = slot + fresh.astype(jnp.int32)
                    carry = jnp.where(fresh, 0.0, carry) + tile_sum
                else:
                    carry = tile_sum
                acc_ref[pl.ds(pl.multiple_of(slot * lead, lead), lead), :bin_dev] = carry
        base = []
        side = lax.div(owner, spaces // 2)
        half = lax.div(lax.axis_index("space"), spaces // 2)
        for r in range(rads):
            place = lax.rem(owner, spaces // 2) * rads + jnp.where(side == half, r, r ^ 1)
            place = spaces // 2 * rads - 1 - place
            base.append((2 * place + side) * rows)
            places = jnp.max(place_ref[pl.ds(group * per, per), :], axis=0, keepdims=True)
            out_ref[pl.ds(base[r] + rows - 1, 1), :] = places
        for f in range(3):
            inner = [jnp.zeros((sub, bin_dev), jnp.float32)] * parts
            for r in range(rads):
                pieces = []
                for a in range(parts):
                    own = acc_ref[pl.ds(a * sub * lead + f * rads + r, sub, stride=lead), :][:, :bin_dev]
                    pieces.append(own + inner[a])
                    inner[a] = inner[a] + jnp.broadcast_to(own[:, bin_dev - 1 :], (sub, bin_dev))
                out_ref[pl.ds(base[r] + f * sub, sub), :] = jnp.concatenate(pieces, axis=1)

    unrolled = acc_ref.shape[0]
    for group in range(unrolled):
        one_group(group, acc_ref.at[group])

    @pl.loop(unrolled, tiles // per)
    def _(group):
        one_group(group, acc_ref.at[0])


def fold(x, height):
    return jnp.concatenate([x[k : k + height] for k in range(0, x.shape[0], height)], axis=1)


def merge_kernel(mine, halo_dev, bin_dev, sub, rows, got_ref, sum_ref):
    sources = got_ref.shape[0] // (2 * rows)
    batch = math.gcd(sources, BATCH)
    parts = LANES // bin_dev
    row_ids = iota((sub, LANES), 0).astype(jnp.float32)
    half = lax.div(lax.axis_index("space"), lax.axis_size("space") // 2)
    side = half if mine else 1 - half

    def add(first):
        picks, values = [], []
        for i in range(batch):
            base = (2 * (first + i) + side) * rows
            places = jnp.broadcast_to(got_ref[pl.ds(base + rows - 1, 1), :], (sub, LANES))
            picks.append((places == row_ids).astype(jnp.float32)[:, : parts * halo_dev])
            pieces = []
            for f in range(3):
                value = got_ref[pl.ds(base + f * sub, sub), :]
                high = value.astype(jnp.bfloat16).astype(jnp.float32)
                pieces.extend([high, value - high])
            values.append(jnp.concatenate(pieces, axis=1))
        pick = jnp.concatenate(picks, axis=0).astype(jnp.bfloat16)
        value = jnp.concatenate(values, axis=0).astype(jnp.bfloat16)
        return matmul(pick, value, (0,))

    sums = lax.fori_loop(1, sources // batch, lambda k, acc: acc + add(k * batch), add(0))
    fields = []
    for f in range(3):
        both = sums[:, 2 * f * LANES : (2 * f + 1) * LANES] + sums[:, (2 * f + 1) * LANES : (2 * f + 2) * LANES]
        acc = None
        for a in range(parts):
            part = both[a * halo_dev : (a + 1) * halo_dev, a * bin_dev : (a + 1) * bin_dev]
            acc = part if acc is None else acc + part
        fields.append(fold(acc, halo_dev // (LANES // bin_dev)))
    sum_ref[...] = jnp.concatenate(fields, axis=0)


def finish_kernel(halo_dev, bin_dev, own_ref, got_ref, mass_ref, volume_ref, entropy_ref, speed_ref):
    total = own_ref[...] + got_ref[...]
    height = halo_dev * bin_dev // LANES
    total = [
        jnp.concatenate(
            [total[f * height : (f + 1) * height, a : a + bin_dev] for a in range(0, LANES, bin_dev)], axis=0
        )
        for f in range(3)
    ]
    mass_ref[...], volume_ref[...], entropy_ref[...] = total
    first = lax.axis_index("rad") * bin_dev + 1
    position = (iota((1, bin_dev), 1) + first).astype(jnp.float32)
    radius = jnp.exp(log_inner + position * (-log_inner / BINS))
    speed_ref[...] = jnp.sqrt(total[0] / radius)


def body(cell_bin, cell_fields, tile_halo, halo_owner):
    spaces = lax.axis_size("space")
    rads = lax.axis_size("rad")
    bin_dev = BINS // rads
    tiles = tile_halo.shape[0]
    halo_dev = halo_owner.shape[0] // spaces
    per = max(2, 2 * tiles // spaces)
    slots = -(-max(1, per // 2) // PACK) * PACK
    sub = slots * bin_dev // LANES
    rows = 3 * sub + 1
    devices = spaces * rads
    vmem = pl.BlockSpec(memory_space=pltpu.VMEM)
    hbm = pl.BlockSpec(memory_space=pltpu.HBM)
    params = pltpu.CompilerParams(vmem_limit_bytes=VMEM_LIMIT)
    outgoing = pl.pallas_call(
        functools.partial(bin_kernel, spaces, rads, per, slots, rows),
        out_shape=jax.ShapeDtypeStruct((devices * rows, LANES), jnp.float32),
        in_specs=[hbm] * 5,
        out_specs=vmem,
        scratch_shapes=[
            pltpu.SMEM(halo_owner.shape, jnp.int32),
            pltpu.SMEM((tiles,), jnp.int32),
            pltpu.VMEM((1, tiles), jnp.int32),
            pltpu.VMEM((tiles, TILE), jnp.int32),
            pltpu.VMEM((tiles, TILE), jnp.int32),
            pltpu.VMEM((tiles, TILE), jnp.float32),
            pltpu.VMEM(cell_fields.shape, jnp.float32),
            pltpu.VMEM((tiles, LANES), jnp.float32),
            pltpu.VMEM((min(UNROLL, tiles // per), slots * FIELDS * rads, LANES), jnp.float32),
            pltpu.SemaphoreType.DMA((5,)),
        ],
        compiler_params=pltpu.CompilerParams(
            vmem_limit_bytes=VMEM_LIMIT
        ),
    )(
        *[
            pltpu.with_memory_space_constraint(x, pltpu.HBM)
            for x in (halo_owner, tile_halo, tile_halo.reshape(1, tiles), cell_bin.reshape(tiles, TILE), cell_fields)
        ]
    )
    order = range(devices // 2 - 1, -1, -1)
    received = lax.all_to_all(
        outgoing.reshape(devices // 2, 2 * rows, 1, LANES),
        ("space", "rad"),
        split_axis=0,
        concat_axis=0,
        axis_index_groups=[[side * (devices // 2) + k for k in order] for side in range(2)],
        tiled=True,
    )
    received = received.reshape(devices * rows, LANES)
    own, other = (
        pl.pallas_call(
            functools.partial(merge_kernel, mine, halo_dev, bin_dev, sub, rows),
            out_shape=jax.ShapeDtypeStruct((3 * halo_dev * bin_dev // LANES, LANES), jnp.float32),
            in_specs=[vmem],
            out_specs=vmem,
            compiler_params=pltpu.CompilerParams(
                vmem_limit_bytes=VMEM_LIMIT
            ),
            cost_estimate=pl.CostEstimate(flops=MERGE_FLOPS, bytes_accessed=devices * rows * LANES * 2, transcendentals=0),
        )(received)
        for mine in (True, False)
    )
    partners = [(d, (d + devices // 2) % devices ^ 1) for d in range(devices)]
    got = lax.ppermute(other, ("space", "rad"), partners)
    return pl.pallas_call(
        functools.partial(finish_kernel, halo_dev, bin_dev),
        out_shape=[jax.ShapeDtypeStruct((halo_dev, bin_dev), jnp.float32)] * 4,
        in_specs=[vmem] * 2,
        out_specs=[vmem] * 4,
        compiler_params=params,
    )(own, got)


def solution(mesh):
    in_specs = (P(("space", "rad")), P(None, ("space", "rad")), P(("space", "rad")), P())
    out_specs = (P("space", "rad"), P("space", "rad"), P("space", "rad"), P("space", "rad"))
    return jax.shard_map(body, mesh=mesh, in_specs=in_specs, out_specs=out_specs, check_vma=False)
```
